32 devices in a mesh: grid: 8 (over z, x), orb: 4 (over y, core).
Axes of the slice: x: 2, y: 2, z: 4, core: 2. Of those that a mesh axis runs over, the one named last changes fastest.
Arguments:
- orbitals: bfloat16 [1800, 65536], P('orb', 'grid'), may hold values from -0.5 to 1.5
- pivots: int32 [3, 96], replicated, may hold values from 0 to 65535, as said below
Outputs:
- cholesky_factor: float32 [65536, 288], P(('grid', 'orb'))
- residual_diagonal: float32 [65536], P(('grid', 'orb'))
- diagonal_peaks: float32 [3], replicated
The draws below stay inside these ranges and needn't reach their ends.
Inputs may be any that keep to these rules, and one draw needn't show every extreme that they name: `pivots`: all 3 x 96 pivot indices are distinct grid points.
All inputs are finite; a program needn't handle non-finite values.
Results may differ from the reference program's by a relative error of at most 0.0003.
Values may be sent and summed in bfloat16 or wider, within the bound.
A program may use at most 64 MiB of HBM per device.

```python
import jax
import jax.numpy as jnp
from jax import lax

ORB = 1800
PIV = 96
STEPS = 3
GRID_POINTS = 65536


def draw_pivots(key, part):
    order = jax.random.permutation(jax.random.fold_in(key, 11), GRID_POINTS)
    return order[:STEPS * PIV].reshape(STEPS, PIV).astype(jnp.int32)


def levels(stream_key, shape, pieces, smallest, largest):
    def one(axis_at, parts):
        draws = jax.random.uniform(jax.random.fold_in(jax.random.fold_in(stream_key, 6), axis_at), (parts,), jnp.float32, smallest / len(pieces), largest / len(pieces))
        return jnp.repeat(jnp.exp(draws), shape[axis_at] // parts).reshape((-1,) + (1,) * (len(shape) - axis_at - 1))

    loudness = one(*pieces[0])
    for cut in pieces[1:]:
        loudness = loudness * one(*cut)
    return loudness


def setup_inputs(seed: int = 0) -> dict:
    keys = jax.random.split(jax.random.key(seed), 3)
    orbitals = jnp.clip(-0.5 + 2.0 * jax.random.uniform(keys[0], (ORB, GRID_POINTS), jnp.float32) ** levels(keys[0], (ORB, GRID_POINTS), ((0, 4), (1, 8)), -0.2, 0.2), -0.5, 1.5).astype(jnp.bfloat16)
    pivots = draw_pivots(jax.random.fold_in(keys[2], 71), 0)
    return dict(orbitals=orbitals, pivots=pivots)


def reference(orbitals, pivots):
    grid_count = orbitals.shape[1]
    squares = jnp.sum(jnp.square(orbitals.astype(jnp.float32)), axis=0)
    diagonal = jnp.square(squares / ORB)
    factor = jnp.zeros((grid_count, STEPS * PIV), jnp.float32)
    peaks = []
    for section in range(STEPS):
        chosen = pivots[section]
        sampled = jnp.take(orbitals, chosen, axis=1)
        known = jnp.take(factor, chosen, axis=0)
        pair = lax.dot_general(sampled.astype(jnp.float32), sampled.astype(jnp.float32), (((0,), (0,)), ((), ())), preferred_element_type=jnp.float32)
        block = jnp.square(pair / ORB) - jnp.dot(known, known.T, precision=lax.Precision.HIGHEST)
        inner = lax.dot_general(orbitals.astype(jnp.float32), sampled.astype(jnp.float32), (((0,), (0,)), ((), ())), preferred_element_type=jnp.float32)
        columns = jnp.square(inner / ORB) - jnp.dot(factor, known.T, precision=lax.Precision.HIGHEST)
        lower = jnp.linalg.cholesky(block)
        fresh = jax.scipy.linalg.solve_triangular(lower, columns.T, lower=True).T
        factor = factor.at[:, section * PIV:(section + 1) * PIV].set(fresh)
        diagonal = diagonal - jnp.sum(fresh * fresh, axis=1)
        peaks.append(jnp.max(diagonal))
    return (factor, diagonal, jnp.stack(peaks))
```

```python
import functools

import jax
import jax.numpy as jnp
from jax import lax
from jax.experimental import pallas as pl
from jax.experimental.pallas import tpu as pltpu
from jax.sharding import PartitionSpec as P

F32 = jnp.float32
BF16 = jnp.bfloat16
HIGHEST = lax.Precision.HIGHEST
MESH = pl.DeviceIdType.MESH
BLOCK = 48
PARTS = 4


def dot_nn(a, b, precision=None):
    return lax.dot_general(
        a, b, (((1,), (0,)), ((), ())), precision=precision, preferred_element_type=F32
    )


def dot_nt(a, b, precision=None):
    return lax.dot_general(
        a, b, (((1,), (1,)), ((), ())), precision=precision, preferred_element_type=F32
    )


def dot_tn(a, b, precision=None):
    return lax.dot_general(
        a, b, (((0,), (0,)), ((), ())), precision=precision, preferred_element_type=F32
    )


def spread_row(t, r):
    return jnp.broadcast_to(t[r : r + 1, :], (8, 128))


def spread_column(t, c):
    return jnp.broadcast_to(t[:, c : c + 1], (8, 128))


def eliminate(square, wide_rows):
    size = square.shape[0]
    groups = size // 8
    width = wide_rows.shape[1] // 128
    tile = [square[8 * i : 8 * i + 8, :] for i in range(groups)]
    wide = [
        [wide_rows[8 * i : 8 * i + 8, 128 * v : 128 * v + 128] for v in range(width)]
        for i in range(groups)
    ]
    row_at = lax.broadcasted_iota(jnp.int32, (8, 128), 0)
    for j in range(groups):
        columns = [spread_column(tile[j], 8 * j + c) for c in range(8)]
        entry = {(r, c): spread_row(columns[c], r) for r in range(8) for c in range(r + 1)}
        scale, low = [], {}
        for k in range(8):
            s = lax.rsqrt(entry[k, k])
            scale.append(s)
            for r in range(k + 1, 8):
                low[r, k] = entry[r, k] * s
            for r in range(k + 1, 8):
                for c in range(k + 1, r + 1):
                    entry[r, c] = entry[r, c] - low[r, k] * low[c, k]

        def forward(rows):
            done = []
            for k in range(8):
                x = rows[k]
                for c in range(k):
                    x = x - low[k, c] * done[c]
                done.append(x * scale[k])
            return done

        def gather(done):
            out = done[0]
            for k in range(1, 8):
                out = jnp.where(row_at == k, done[k], out)
            return out

        last = j == groups - 1
        fresh_tile = None if last else forward([spread_row(tile[j], k) for k in range(8)])
        fresh_wide = [forward([spread_row(wide[j][v], k) for k in range(8)]) for v in range(width)]
        for i in range(j + 1, groups):
            left = forward([spread_column(tile[i], 8 * j + c) for c in range(8)])
            for k in range(8):
                tile[i] = tile[i] - left[k] * fresh_tile[k]
                for v in range(width):
                    wide[i][v] = wide[i][v] - left[k] * fresh_wide[v][k]
        for v in range(width):
            wide[j][v] = gather(fresh_wide[v])
    return jnp.concatenate([jnp.concatenate(row, axis=1) for row in wide], axis=0)


def kernel(
    n_grid, n_orb, steps, orbitals_count,
    orb_hbm, piv_ref,
    factor_hbm, diag_ref, peaks_ref,
    own, other, mine, total, heard, swap, sums, arrived, side_sums, side_arrived, local, pair_send, pair_recv,
    aug, out_v, tile_mine, tile_orb, tile_grid,
    load_sem, out_sem, x_send, x_recv, p1_send, p1_recv, p2_send, p2_recv,
    c_send, c_recv, q_send, q_recv, h_send, h_recv, s_send, s_recv, z_send, z_recv,
    mo_send, mo_recv, mg_send, mg_recv,
):
    g = lax.axis_index("grid")
    o = lax.axis_index("orb")
    core = lax.rem(o, 2)
    side = o // 2
    mate = o + 1 - 2 * core
    across = (1 - side) * 2 + core
    share = own.shape[2]
    slots, slot_rows, _ = mine.shape
    rank = slots * slot_rows
    part = share // PARTS
    rows = share * n_orb
    loads = []
    for b in range(n_orb):
        copy = pltpu.make_async_copy(
            orb_hbm.at[:, pl.ds(b * share, share)], own.at[b], load_sem.at[b]
        )
        copy.start()
        loads.append(copy)
    barrier = pltpu.get_barrier_semaphore()
    for d in range(1, n_grid):
        pl.semaphore_signal(
            barrier, inc=1, device_id=(lax.rem(g + d, n_grid), o), device_id_type=MESH
        )
    for d in range(1, n_orb):
        pl.semaphore_signal(
            barrier, inc=1, device_id=(g, lax.rem(o + d, n_orb)), device_id_type=MESH
        )
    base = g * rows
    flat = jnp.concatenate(
        [piv_ref[...].astype(F32), jnp.zeros((8 - piv_ref.shape[0], piv_ref.shape[1]), F32)], axis=0
    ).T
    wanted = (
        jnp.concatenate([flat[:, s : s + 1] for s in range(steps)], axis=0).astype(jnp.int32)
        - base
    )
    picked = None
    for b in range(n_orb):
        loads[b].wait()
        lanes = lax.broadcasted_iota(jnp.int32, (rank, share), 1) + b * share
        hot = jnp.where(lanes == wanted, 1.0, 0.0).astype(BF16)
        term = dot_nt(hot, own[b])
        picked = term if picked is None else picked + term
    picked = picked.astype(BF16)
    for s in range(slots):
        mine[s] = picked[s * slot_rows : (s + 1) * slot_rows]
    pl.semaphore_wait(barrier, n_grid + n_orb - 2)
    def first(d):
        target = lax.rem(g + d, n_grid)
        return target, pltpu.make_async_remote_copy(
            src_ref=mine.at[lax.rem(target, slots)],
            dst_ref=heard.at[d],
            send_sem=p1_send.at[d],
            recv_sem=p1_recv.at[d],
            device_id=(target, o),
            device_id_type=MESH,
        )

    def second(d):
        target = lax.rem(g + d, n_grid)
        return pltpu.make_async_remote_copy(
            src_ref=heard.at[0],
            dst_ref=total.at[lax.rem(g, slots)],
            send_sem=p2_send.at[d],
            recv_sem=p2_recv.at[d],
            device_id=(target, o),
            device_id_type=MESH,
        )
    for d in range(1, n_grid):
        target, copy = first(d)

        @pl.when(target < slots)
        def _(copy=copy):
            copy.start()
    crossing = []
    for yy in range(2):
        start = pl.multiple_of((yy * 2 + 1 - core) * share, share)
        copy = pltpu.make_async_remote_copy(
            src_ref=orb_hbm.at[:, pl.ds(start, share)],
            dst_ref=other.at[yy],
            send_sem=x_send.at[yy],
            recv_sem=x_recv.at[yy],
            device_id=(g, mate),
            device_id_type=MESH,
        )
        copy.start()
        crossing.append(copy)
    @pl.when(g < slots)
    def _():
        added = mine[lax.rem(g, slots)]
        for d in range(1, n_grid):
            first(d)[1].wait_recv()
            added = added + heard[d]
        heard[0] = added
        for d in range(1, n_grid):
            second(d).start()
        total[lax.rem(g, slots)] = added
    for copy in crossing:
        copy.wait_recv()

    def moments(block, yy, p):
        lo = p * part
        a = own[block, :, lo : lo + part]
        b = other[yy, :, lo : lo + part]
        a32 = a.astype(F32)
        b32 = b.astype(F32)
        squares = jnp.sum(a32 * a32, axis=0, keepdims=True) + jnp.sum(
            b32 * b32, axis=0, keepdims=True
        )
        point_sum = jnp.sum(a32, axis=0, keepdims=True) + jnp.sum(b32, axis=0, keepdims=True)
        return squares, point_sum
    for p in range(PARTS):
        squares, point_sum = moments(across, 1 - side, p)
        side_sums[p] = jnp.zeros((8, part), F32)
        side_sums[p, 0:1] = squares
        side_sums[p, 1:2] = point_sum
        squares, _ = moments(o, side, p)
        local[p, rank : rank + 8, :] = jnp.broadcast_to(squares, (8, part))
    for d in range(1, n_grid):
        source = lax.rem(g + n_grid - d, n_grid)

        @pl.when(source < slots)
        def _(d=d):
            second(d).wait_recv()
    swap_copy = pltpu.make_async_remote_copy(
        src_ref=total, dst_ref=swap, send_sem=c_send, recv_sem=c_recv,
        device_id=(g, mate), device_id_type=MESH,
    )
    swap_copy.start()
    here = jnp.reshape(total[...], (rank, total.shape[2]))
    pair_here = dot_nt(here, here)
    swap_copy.wait_recv()
    there = jnp.reshape(swap[...], (rank, swap.shape[2]))
    pair = pair_here + dot_nt(there, there)
    half = rank // 2
    pivot_mean = (
        jnp.sum(here.astype(F32), axis=1, keepdims=True)
        + jnp.sum(there.astype(F32), axis=1, keepdims=True)
    ) / (2.0 * total.shape[2])
    for h in range(2):
        pair_send[h, :, 0:rank] = pair[h * half : (h + 1) * half]
        pair_send[h, :, rank : rank + 1] = pivot_mean[h * half : (h + 1) * half]
    pair_copy = pltpu.make_async_remote_copy(
        src_ref=pair_send.at[core], dst_ref=pair_recv.at[0], send_sem=q_send, recv_sem=q_recv,
        device_id=(g, across), device_id_type=MESH,
    )
    pair_copy.start()

    def products(block, yy, p):
        lo = p * part
        a = own[block, :, lo : lo + part]
        b = other[yy, :, lo : lo + part]
        return dot_nn(here, a) + dot_nn(there, b)
    travel = []
    for p in range(PARTS):
        inner = products(across, 1 - side, p)
        squares = side_sums[p, 0:1]
        point_sum = side_sums[p, 1:2]
        rest = inner - pivot_mean * point_sum
        most = jnp.max(jnp.abs(rest), axis=0, keepdims=True)
        step = jnp.maximum(most * (1.0 / 32767.0), 1e-30)
        coded = jnp.round(rest * (1.0 / step))
        sums[p] = jnp.clip(coded, -32767.0, 32767.0).astype(jnp.int32).astype(jnp.int16)
        side_sums[p, 2:3] = step
        for copy in (
            pltpu.make_async_remote_copy(
                src_ref=side_sums.at[p], dst_ref=side_arrived.at[p],
                send_sem=z_send.at[p], recv_sem=z_recv.at[p],
                device_id=(g, across), device_id_type=MESH,
            ),
            pltpu.make_async_remote_copy(
                src_ref=sums.at[p], dst_ref=arrived.at[p],
                send_sem=s_send.at[p], recv_sem=s_recv.at[p],
                device_id=(g, across), device_id_type=MESH,
            ),
        ):
            copy.start()
            travel.append(copy)
    pair_copy.wait_recv()
    half_copy = pltpu.make_async_remote_copy(
        src_ref=pair_recv.at[0], dst_ref=pair_recv.at[1], send_sem=h_send, recv_sem=h_recv,
        device_id=(g, mate), device_id_type=MESH,
    )
    half_copy.start()
    for p in range(PARTS):
        local[p, 0:rank, :] = products(o, side, p)
    half_copy.wait_recv()
    first_half = jnp.where(core == 0, pair_recv[0], pair_recv[1])
    second_half = jnp.where(core == 0, pair_recv[1], pair_recv[0])
    wide = aug.shape[1]
    aug[...] = jnp.zeros((rank, wide), F32)
    aug[0:half, 0:rank] = jnp.square((pair_send[0] + first_half)[:, 0:rank] / orbitals_count)
    aug[half:rank, 0:rank] = jnp.square((pair_send[1] + second_half)[:, 0:rank] / orbitals_count)
    far_mean = jnp.concatenate(
        [first_half[:, rank : rank + 1], second_half[:, rank : rank + 1]], axis=0
    )

    for j in range(rank // BLOCK):
        start = j * BLOCK
        at = lax.broadcasted_iota(jnp.int32, (BLOCK, wide), 1)
        strip = jnp.where(at >= start, aug[start : start + BLOCK, :], 0.0)
        if j:
            low_edge = start // 128 * 128
            high_edge = -(-(start + BLOCK) // 128) * 128
            done = jnp.concatenate(
                [
                    jnp.where(
                        (at >= start) | (at < i + BLOCK), aug[i : i + BLOCK, :], 0.0
                    )
                    for i in range(0, start, BLOCK)
                ],
                axis=0,
            )
            above = dot_tn(aug[0:start, low_edge:high_edge], done, HIGHEST)
            strip = strip - above[start - low_edge : start - low_edge + BLOCK, :]
        square = pltpu.roll(strip, wide - start, 1) if j else strip
        square = square[:, 0:128]
        unit = jnp.where(at == lax.broadcasted_iota(jnp.int32, (BLOCK, wide), 0) + start, 1.0, 0.0)
        solved = eliminate(square, jnp.where((at >= start) & (at < start + BLOCK), unit, strip))
        aug[start : start + BLOCK, :] = solved
    lower_inverse = jnp.concatenate(
        [
            jnp.where(at < i + BLOCK, aug[i : i + BLOCK, :], 0.0)
            for i in range(0, rank, BLOCK)
        ],
        axis=0,
    )

    count = rank // steps
    best = [None] * steps
    stores = []
    for p in range(PARTS):
        travel[2 * p].wait_recv()
        travel[2 * p + 1].wait_recv()
        far = side_arrived[p]
        inner = (
            local[p, 0:rank, :]
            + arrived[p].astype(jnp.int32).astype(F32) * far[2:3]
            + far_mean * far[1:2]
        )
        columns = jnp.square(inner / orbitals_count)
        diagonal = jnp.square((local[p, rank : rank + 1, :] + far[0:1]) / orbitals_count)
        solved = dot_nn(lower_inverse[:, 0:rank], columns, HIGHEST)
        out_v[p] = solved
        store = pltpu.make_async_copy(
            out_v.at[p], factor_hbm.at[:, pl.ds(p * part, part)], out_sem.at[p]
        )
        store.start()
        stores.append(store)
        for s in range(steps):
            piece = solved[s * count : (s + 1) * count]
            diagonal = diagonal - jnp.sum(piece * piece, axis=0, keepdims=True)
            best[s] = diagonal if best[s] is None else jnp.maximum(best[s], diagonal)
        diag_ref[:, p * part : (p + 1) * part] = diagonal
    row8 = lax.broadcasted_iota(jnp.int32, (8, 128), 0)
    tile = jnp.zeros((8, 128), F32)
    for s in range(steps):
        top = jnp.max(best[s], axis=1, keepdims=True)
        tile = jnp.where(row8 == s, jnp.broadcast_to(top, (8, 128)), tile)
    tile_mine[0] = tile
    round_orb = []
    for d in range(1, n_orb):
        copy = pltpu.make_async_remote_copy(
            src_ref=tile_mine.at[0], dst_ref=tile_orb.at[d],
            send_sem=mo_send.at[d], recv_sem=mo_recv.at[d],
            device_id=(g, lax.rem(o + d, n_orb)), device_id_type=MESH,
        )
        copy.start()
        round_orb.append(copy)
    for d in range(1, n_orb):
        round_orb[d - 1].wait_recv()
        tile = jnp.maximum(tile, tile_orb[d])
    tile_mine[1] = tile
    round_grid = []
    for d in range(1, n_grid):
        copy = pltpu.make_async_remote_copy(
            src_ref=tile_mine.at[1], dst_ref=tile_grid.at[d],
            send_sem=mg_send.at[d], recv_sem=mg_recv.at[d],
            device_id=(lax.rem(g + d, n_grid), o), device_id_type=MESH,
        )
        copy.start()
        round_grid.append(copy)
    for d in range(1, n_grid):
        round_grid[d - 1].wait_recv()
        tile = jnp.maximum(tile, tile_grid[d])
    peaks_ref[...] = tile
    for store in stores:
        store.wait()
    for d in range(1, n_grid):
        target, copy = first(d)

        @pl.when(target < slots)
        def _(copy=copy):
            copy.wait_send()

    @pl.when(g < slots)
    def _():
        for d in range(1, n_grid):
            second(d).wait_send()

    for copy in crossing + [swap_copy, pair_copy, half_copy] + travel + round_orb + round_grid:
        copy.wait_send()


def solution(mesh):
    n_grid, n_orb = mesh.shape["grid"], mesh.shape["orb"]
    assert n_orb == 4

    def on_device(orbitals, pivots):
        depth, rows = orbitals.shape
        steps, count = pivots.shape
        rank = steps * count
        share = rows // n_orb
        part = share // PARTS
        slot_rows = -(-rank // n_grid)
        slot_rows = -(-slot_rows // 16) * 16
        while rank % slot_rows:
            slot_rows += 16
        slots = rank // slot_rows
        wide = -(-rank // 128) * 128
        dma = pltpu.SemaphoreType.DMA
        vmem = pltpu.VMEM
        factor, diagonal, peaks = pl.pallas_call(
            functools.partial(kernel, n_grid, n_orb, steps, depth * n_orb),
            out_shape=(
                jax.ShapeDtypeStruct((rank, share), F32),
                jax.ShapeDtypeStruct((1, share), F32),
                jax.ShapeDtypeStruct((8, 128), F32),
            ),
            in_specs=[
                pl.BlockSpec(memory_space=pl.ANY),
                pl.BlockSpec(memory_space=vmem),
            ],
            out_specs=(
                pl.BlockSpec(memory_space=pl.ANY),
                pl.BlockSpec(memory_space=vmem),
                pl.BlockSpec(memory_space=vmem),
            ),
            scratch_shapes=[
                vmem((n_orb, depth, share), BF16),
                vmem((2, depth, share), BF16),
                vmem((slots, slot_rows, depth), BF16),
                vmem((slots, slot_rows, depth), BF16),
                vmem((n_grid, slot_rows, depth), BF16),
                vmem((slots, slot_rows, depth), BF16),
                vmem((PARTS, rank, part), jnp.int16),
                vmem((PARTS, rank, part), jnp.int16),
                vmem((PARTS, 8, part), F32),
                vmem((PARTS, 8, part), F32),
                vmem((PARTS, rank + 8, part), F32),
                vmem((2, rank // 2, rank + 1), F32),
                vmem((2, rank // 2, rank + 1), F32),
                vmem((rank, wide), F32),
                vmem((PARTS, rank, part), F32),
                vmem((2, 8, 128), F32),
                vmem((n_orb, 8, 128), F32),
                vmem((n_grid, 8, 128), F32),
                dma((n_orb,)), dma((PARTS,)), dma((2,)), dma((2,)),
                dma((n_grid,)), dma((n_grid,)), dma((n_grid,)), dma((n_grid,)),
                dma, dma, dma, dma, dma, dma, dma((PARTS,)), dma((PARTS,)),
                dma((PARTS,)), dma((PARTS,)),
                dma((n_orb,)), dma((n_orb,)), dma((n_grid,)), dma((n_grid,)),
            ],
            compiler_params=pltpu.CompilerParams(
                collective_id=0, has_side_effects=True, vmem_limit_bytes=58 * 1024 * 1024
            ),
        )(orbitals, pivots)
        return factor.T, diagonal.reshape(share), peaks[:steps, 0]

    return jax.shard_map(
        on_device,
        mesh=mesh,
        in_specs=(P("orb", "grid"), P()),
        out_specs=(P(("grid", "orb"), None), P(("grid", "orb")), P()),
        check_vma=False,
    )
```

```python
import functools

import jax
import jax.numpy as jnp
from jax import lax
from jax.experimental import pallas as pl
from jax.experimental.pallas import tpu as pltpu
from jax.sharding import PartitionSpec as P

F32 = jnp.float32
BF16 = jnp.bfloat16
HIGHEST = lax.Precision.HIGHEST
MESH = pl.DeviceIdType.MESH
BLOCK = 48
AHEAD = 2


def dot_nn(a, b, precision=None):
    return lax.dot_general(
        a, b, (((1,), (0,)), ((), ())), precision=precision, preferred_element_type=F32
    )


def dot_nt(a, b, precision=None):
    return lax.dot_general(
        a, b, (((1,), (1,)), ((), ())), precision=precision, preferred_element_type=F32
    )


def dot_tn(a, b, precision=None):
    return lax.dot_general(
        a, b, (((0,), (0,)), ((), ())), precision=precision, preferred_element_type=F32
    )


def spread_row(t, r):
    return jnp.broadcast_to(t[r : r + 1, :], (8, 128))


def spread_column(t, c):
    return jnp.broadcast_to(t[:, c : c + 1], (8, 128))


def eliminate(square, wide_rows):
    size = square.shape[0]
    groups = size // 8
    width = wide_rows.shape[1] // 128
    tile = [square[8 * i : 8 * i + 8, :] for i in range(groups)]
    wide = [
        [wide_rows[8 * i : 8 * i + 8, 128 * v : 128 * v + 128] for v in range(width)]
        for i in range(groups)
    ]
    row_at = lax.broadcasted_iota(jnp.int32, (8, 128), 0)
    for j in range(groups):
        columns = [spread_column(tile[j], 8 * j + c) for c in range(8)]
        entry = {(r, c): spread_row(columns[c], r) for r in range(8) for c in range(r + 1)}
        scale, low = [], {}
        for k in range(8):
            s = lax.rsqrt(entry[k, k])
            scale.append(s)
            for r in range(k + 1, 8):
                low[r, k] = entry[r, k] * s
            for r in range(k + 1, 8):
                for c in range(k + 1, r + 1):
                    entry[r, c] = entry[r, c] - low[r, k] * low[c, k]

        def forward(rows):
            done = []
            for k in range(8):
                x = rows[k]
                for c in range(k):
                    x = x - low[k, c] * done[c]
                done.append(x * scale[k])
            return done

        def gather(done):
            out = done[0]
            for k in range(1, 8):
                out = jnp.where(row_at == k, done[k], out)
            return out

        last = j == groups - 1
        fresh_tile = None if last else forward([spread_row(tile[j], k) for k in range(8)])
        fresh_wide = [forward([spread_row(wide[j][v], k) for k in range(8)]) for v in range(width)]
        for i in range(j + 1, groups):
            left = forward([spread_column(tile[i], 8 * j + c) for c in range(8)])
            for k in range(8):
                tile[i] = tile[i] - left[k] * fresh_tile[k]
                for v in range(width):
                    wide[i][v] = wide[i][v] - left[k] * fresh_wide[v][k]
        for v in range(width):
            wide[j][v] = gather(fresh_wide[v])
    return jnp.concatenate([jnp.concatenate(row, axis=1) for row in wide], axis=0)


def layout(rank, count, depth, n_grid):
    groups = [(0, count), (count, rank - count)] if rank > count else [(0, rank)]
    tiles = -(-depth // 128)
    cuts = []
    for _, rows in groups:
        parts = max(
            (r for r in range(1, rows // 16 + 1) if r * tiles <= n_grid and rows % (16 * r) == 0),
            default=1,
        )
        cuts.append((parts, rows // parts))
    return groups, tiles, cuts


def pieces_of(share):
    units = share // 128
    sizes = [units * 5 // 16, units * 5 // 16, units * 4 // 16]
    sizes.append(units - sum(sizes))
    starts = [sum(sizes[:i]) for i in range(len(sizes))]
    return [(128 * a, 128 * n) for a, n in zip(starts, sizes) if n]


def kernel(
    n_grid, n_orb, steps, orbitals_count, plan,
    orb_hbm, piv_hbm,
    factor_hbm, diag_ref, peaks_ref,
    piv_ref, own, other, mines, totals, heards, swaps, sums, arrived, scales, far_scales,
    moment, far_moment, local, own_squares, pair_send, pair_recv,
    aug, out_v, tile_mine, tile_orb, tile_grid,
    piv_sem, load_sem, out_sem, x_send, x_recv, p1_send, p1_recv, p2_send, p2_recv,
    c_send, c_recv, q_send, q_recv, h_send, h_recv, s_send, s_recv, z_send, z_recv,
    m_send, m_recv, mo_send, mo_recv, mg_send, mg_recv,
):
    groups, tiles, cuts = plan
    g = lax.axis_index("grid")
    o = lax.axis_index("orb")
    core = lax.rem(o, 2)
    side = o // 2
    mate = o + 1 - 2 * core
    across = (1 - side) * 2 + core
    depth, share = own.shape[1], own.shape[2]
    count = piv_ref.shape[1]
    rank = steps * count
    rows = share * n_orb
    pieces = pieces_of(share)
    n_groups = len(groups)
    piv_copy = pltpu.make_async_copy(piv_hbm, piv_ref, piv_sem)
    piv_copy.start()
    loads = []
    for b in range(n_orb):
        copy = pltpu.make_async_copy(
            orb_hbm.at[:, pl.ds(b * share, share)], own.at[b], load_sem.at[b]
        )
        copy.start()
        loads.append(copy)

    barrier = pltpu.get_barrier_semaphore()
    for d in range(1, n_grid):
        pl.semaphore_signal(
            barrier, inc=1, device_id=(lax.rem(g + d, n_grid), o), device_id_type=MESH
        )
    for d in range(1, n_orb):
        pl.semaphore_signal(
            barrier, inc=1, device_id=(g, lax.rem(o + d, n_orb)), device_id_type=MESH
        )
    piv_copy.wait()
    base = g * rows
    flat = jnp.concatenate(
        [piv_ref[...].astype(F32), jnp.zeros((8 - piv_ref.shape[0], count), F32)], axis=0
    ).T
    wanted = (
        jnp.concatenate([flat[:, s : s + 1] for s in range(steps)], axis=0).astype(jnp.int32)
        - base
    )
    picked = None
    for b in range(n_orb):
        loads[b].wait()
        lanes = lax.broadcasted_iota(jnp.int32, (rank, share), 1) + b * share
        hot = jnp.where(lanes == wanted, 1.0, 0.0).astype(BF16)
        term = dot_nt(hot, own[b])
        picked = term if picked is None else picked + term
    picked = jnp.concatenate(
        [picked.astype(BF16), jnp.zeros((rank, tiles * 128 - depth), BF16)], axis=1
    )
    for i, (first_row, _) in enumerate(groups):
        parts, size = cuts[i]
        for q in range(parts * tiles):
            at = first_row + q // tiles * size
            lane = q % tiles * 128
            mines[i][q] = picked[at : at + size, lane : lane + 128]
    pl.semaphore_wait(barrier, n_grid + n_orb - 2)

    def block_of(i, owner):
        return lax.rem(owner, cuts[i][0] * tiles)

    def owned(i, owner, action):
        if cuts[i][0] * tiles == n_grid:
            action()
        else:
            pl.when(owner < cuts[i][0] * tiles)(action)

    def first(i, d):
        target = lax.rem(g + d, n_grid)
        return target, pltpu.make_async_remote_copy(
            src_ref=mines[i].at[block_of(i, target)],
            dst_ref=heards[i].at[d],
            send_sem=p1_send.at[i, d],
            recv_sem=p1_recv.at[i, d],
            device_id=(target, o),
            device_id_type=MESH,
        )

    def second(i, d):
        target = lax.rem(g + d, n_grid)
        return pltpu.make_async_remote_copy(
            src_ref=heards[i].at[0],
            dst_ref=totals[i].at[block_of(i, g)],
            send_sem=p2_send.at[i, d],
            recv_sem=p2_recv.at[i, d],
            device_id=(target, o),
            device_id_type=MESH,
        )
    for i in range(n_groups):
        for d in range(1, n_grid):
            target, copy = first(i, d)
            owned(i, target, copy.start)

    crossing = []
    for yy in range(2):
        start = pl.multiple_of((yy * 2 + 1 - core) * share, share)
        copy = pltpu.make_async_remote_copy(
            src_ref=orb_hbm.at[:, pl.ds(start, share)],
            dst_ref=other.at[yy],
            send_sem=x_send.at[yy],
            recv_sem=x_recv.at[yy],
            device_id=(g, mate),
            device_id_type=MESH,
        )
        copy.start()
        crossing.append(copy)

    for i in range(n_groups):

        def add_up(i=i):
            added = mines[i][block_of(i, g)]
            for d in range(1, n_grid):
                first(i, d)[1].wait_recv()
                added = added + heards[i][d]
            heards[i][0] = added
            for d in range(1, n_grid):
                second(i, d).start()
            totals[i][block_of(i, g)] = added

        owned(i, g, add_up)
    for copy in crossing:
        copy.wait_recv()

    def squares_of(block):
        x = block.astype(F32)
        return jnp.sum(x * x, axis=0, keepdims=True)

    def sum_of(block):
        return jnp.sum(block.astype(F32), axis=0, keepdims=True)

    for lo, n in pieces:
        a, b = own[across, :, lo : lo + n], other[1 - side, :, lo : lo + n]
        moment[:, lo : lo + n] = squares_of(a) + squares_of(b)
        moment[:, share + lo : share + lo + n] = sum_of(a) + sum_of(b)
    moment_copy = pltpu.make_async_remote_copy(
        src_ref=moment, dst_ref=far_moment, send_sem=m_send, recv_sem=m_recv,
        device_id=(g, across), device_id_type=MESH,
    )
    moment_copy.start()

    def gathered(i, ref):
        parts, _ = cuts[i]
        return jnp.concatenate(
            [
                jnp.concatenate([ref[r * tiles + t] for t in range(tiles)], axis=1)
                for r in range(parts)
            ],
            axis=0,
        )[:, 0:depth]

    swapping, here, there, means = [], [], [], []

    def meet(i):
        for d in range(1, n_grid):
            source = lax.rem(g + n_grid - d, n_grid)
            owned(i, source, second(i, d).wait_recv)
        copy = pltpu.make_async_remote_copy(
            src_ref=totals[i], dst_ref=swaps[i], send_sem=c_send.at[i], recv_sem=c_recv.at[i],
            device_id=(g, mate), device_id_type=MESH,
        )
        copy.start()
        swapping.append(copy)
        here.append(gathered(i, totals[i]))
        copy.wait_recv()
        there.append(gathered(i, swaps[i]))
        means.append(
            (
                jnp.sum(here[i].astype(F32), axis=1, keepdims=True)
                + jnp.sum(there[i].astype(F32), axis=1, keepdims=True)
            )
            / (2.0 * depth)
        )

    travel = {}

    def code(i, p):
        lo, n = pieces[p]
        top, size = groups[i]
        inner = dot_nn(here[i], own[across, :, lo : lo + n]) + dot_nn(
            there[i], other[1 - side, :, lo : lo + n]
        )
        rest = inner - means[i] * moment[:, share + lo : share + lo + n]
        most = jnp.max(jnp.abs(rest), axis=0, keepdims=True)
        step = jnp.maximum(most * (1.0 / 32767.0), 1e-30)
        coded = jnp.clip(jnp.round(rest * (1.0 / step)), -32767.0, 32767.0)
        sums[top : top + size, lo : lo + n] = coded.astype(jnp.int32).astype(jnp.int16)
        scales[:, i * share + lo : i * share + lo + n] = step

    def send(i, p):
        lo, n = pieces[p]
        top, size = groups[i]
        travel[i, p] = (
            pltpu.make_async_remote_copy(
                src_ref=scales.at[:, pl.ds(i * share + lo, n)],
                dst_ref=far_scales.at[:, pl.ds(i * share + lo, n)],
                send_sem=z_send.at[i, p], recv_sem=z_recv.at[i, p],
                device_id=(g, across), device_id_type=MESH,
            ),
            pltpu.make_async_remote_copy(
                src_ref=sums.at[pl.ds(top, size), pl.ds(lo, n)],
                dst_ref=arrived.at[pl.ds(top, size), pl.ds(lo, n)],
                send_sem=s_send.at[i, p], recv_sem=s_recv.at[i, p],
                device_id=(g, across), device_id_type=MESH,
            ),
        )
        for copy in travel[i, p]:
            copy.start()

    late = n_groups - 1
    for i in range(late):
        meet(i)
        for p in range(len(pieces)):
            code(i, p)
            if i or p < AHEAD:
                send(i, p)
    meet(late)
    here_all = jnp.concatenate(here, axis=0)
    there_all = jnp.concatenate(there, axis=0)
    mean_all = jnp.concatenate(means, axis=0)
    pair = dot_nt(here_all, here_all) + dot_nt(there_all, there_all)
    corners = [(r, c) for r in range(steps) for c in range(r, steps)]
    half = len(corners) // 2

    def corner(r, c):
        return pair[r * count : (r + 1) * count, c * count : (c + 1) * count]

    for k, (r, c) in enumerate(corners):
        pair_send[k // half, k % half, :, 0:count] = corner(r, c)
        pair_send[k // half, k % half, :, count : count + 1] = mean_all[
            r * count : (r + 1) * count
        ]
    pair_copy = pltpu.make_async_remote_copy(
        src_ref=pair_send.at[core], dst_ref=pair_recv.at[0], send_sem=q_send, recv_sem=q_recv,
        device_id=(g, across), device_id_type=MESH,
    )
    pair_copy.start()
    if late:
        for p in range(AHEAD, len(pieces)):
            send(0, p)
    for p in range(len(pieces)):
        code(late, p)
        send(late, p)
    for lo, n in pieces:
        a, b = own[o, :, lo : lo + n], other[side, :, lo : lo + n]
        local[:, lo : lo + n] = dot_nn(here_all, a) + dot_nn(there_all, b)
        own_squares[:, lo : lo + n] = squares_of(a) + squares_of(b)
    pair_copy.wait_recv()
    half_copy = pltpu.make_async_remote_copy(
        src_ref=pair_recv.at[0], dst_ref=pair_recv.at[1], send_sem=h_send, recv_sem=h_recv,
        device_id=(g, mate), device_id_type=MESH,
    )
    half_copy.start()
    half_copy.wait_recv()
    wide = aug.shape[1]
    aug[...] = jnp.zeros((rank, wide), F32)
    far_means = [None] * steps
    for k, (r, c) in enumerate(corners):
        which = core if k < half else 1 - core
        far = pair_recv[which, k % half]
        aug[r * count : (r + 1) * count, 128 * c : 128 * c + count] = jnp.square(
            (pair_send[k // half, k % half] + far)[:, 0:count] / orbitals_count
        )
        far_means[r] = far[:, count : count + 1]
    far_mean = jnp.concatenate(far_means, axis=0)

    def lane_of(row):
        return row // count * 128 + row % count

    at = lax.broadcasted_iota(jnp.int32, (BLOCK, wide), 1)
    eye_row = lax.broadcasted_iota(jnp.int32, (BLOCK, wide), 0)
    for start in range(0, rank, BLOCK):
        lane = lane_of(start)
        tile = lane // 128 * 128
        strip = jnp.where(at >= lane, aug[start : start + BLOCK, :], 0.0)
        if start:
            done = jnp.concatenate(
                [
                    jnp.where(
                        (at >= lane) | (at < lane_of(i) + BLOCK), aug[i : i + BLOCK, :], 0.0
                    )
                    for i in range(0, start, BLOCK)
                ],
                axis=0,
            )
            above = dot_tn(aug[0:start, tile : tile + 128], done, HIGHEST)
            strip = strip - above[lane - tile : lane - tile + BLOCK, :]
        square = strip[:, tile : tile + 128]
        if lane > tile:
            square = pltpu.roll(square, 128 - (lane - tile), 1)
        unit = jnp.where(at == eye_row + lane, 1.0, 0.0)
        aug[start : start + BLOCK, :] = eliminate(
            square, jnp.where((at >= lane) & (at < lane + BLOCK), unit, strip)
        )
    inverse = []
    for s in range(steps):
        bands = []
        for i in range(s * count, (s + 1) * count, BLOCK):
            bands.append(jnp.where(at < lane_of(i) + BLOCK, aug[i : i + BLOCK, :], 0.0))
        band = jnp.concatenate(bands, axis=0)
        inverse.append(
            jnp.concatenate([band[:, 128 * c : 128 * c + count] for c in range(s + 1)], axis=1)
        )

    best = [None] * steps
    stores = []
    moment_copy.wait_recv()
    for p, (lo, n) in enumerate(pieces):
        for i in range(n_groups):
            for copy in travel[i, p]:
                copy.wait_recv()
        scale = jnp.concatenate(
            [
                jnp.broadcast_to(
                    far_scales[:, i * share + lo : i * share + lo + n], (size, n)
                )
                for i, (_, size) in enumerate(groups)
            ],
            axis=0,
        )
        inner = (
            local[:, lo : lo + n]
            + arrived[:, lo : lo + n].astype(jnp.int32).astype(F32) * scale
            + far_mean * far_moment[:, share + lo : share + lo + n]
        )
        columns = jnp.square(inner / orbitals_count)
        diagonal = jnp.square(
            (own_squares[:, lo : lo + n] + far_moment[:, lo : lo + n]) / orbitals_count
        )
        for s in range(steps):
            solved = dot_nn(inverse[s], columns[0 : (s + 1) * count], HIGHEST)
            out_v[s * count : (s + 1) * count, lo : lo + n] = solved
            diagonal = diagonal - jnp.sum(solved * solved, axis=0, keepdims=True)
            top = jnp.max(diagonal, axis=1, keepdims=True)
            best[s] = top if best[s] is None else jnp.maximum(best[s], top)
        store = pltpu.make_async_copy(
            out_v.at[:, pl.ds(lo, n)], factor_hbm.at[:, pl.ds(lo, n)], out_sem.at[p]
        )
        store.start()
        stores.append(store)
        diag_ref[:, lo : lo + n] = diagonal
    row8 = lax.broadcasted_iota(jnp.int32, (8, 128), 0)
    tile = jnp.zeros((8, 128), F32)
    for s in range(steps):
        tile = jnp.where(row8 == s, jnp.broadcast_to(best[s], (8, 128)), tile)
    tile_mine[0] = tile
    round_orb = []
    for d in range(1, n_orb):
        copy = pltpu.make_async_remote_copy(
            src_ref=tile_mine.at[0], dst_ref=tile_orb.at[d],
            send_sem=mo_send.at[d], recv_sem=mo_recv.at[d],
            device_id=(g, lax.rem(o + d, n_orb)), device_id_type=MESH,
        )
        copy.start()
        round_orb.append(copy)
    for d in range(1, n_orb):
        round_orb[d - 1].wait_recv()
        tile = jnp.maximum(tile, tile_orb[d])
    tile_mine[1] = tile
    round_grid = []
    for d in range(1, n_grid):
        copy = pltpu.make_async_remote_copy(
            src_ref=tile_mine.at[1], dst_ref=tile_grid.at[d],
            send_sem=mg_send.at[d], recv_sem=mg_recv.at[d],
            device_id=(lax.rem(g + d, n_grid), o), device_id_type=MESH,
        )
        copy.start()
        round_grid.append(copy)
    for d in range(1, n_grid):
        round_grid[d - 1].wait_recv()
        tile = jnp.maximum(tile, tile_grid[d])
    peaks_ref[...] = tile
    for store in stores:
        store.wait()
    for i in range(n_groups):
        for d in range(1, n_grid):
            target, copy = first(i, d)
            owned(i, target, copy.wait_send)

        def sent(i=i):
            for d in range(1, n_grid):
                second(i, d).wait_send()

        owned(i, g, sent)

    for copy in crossing + swapping + [moment_copy, pair_copy, half_copy] + round_orb + round_grid:
        copy.wait_send()
    for pair_of in travel.values():
        for copy in pair_of:
            copy.wait_send()


def solution(mesh):
    n_grid, n_orb = mesh.shape["grid"], mesh.shape["orb"]
    assert n_orb == 4

    def on_device(orbitals, pivots):
        depth, rows = orbitals.shape
        steps, count = pivots.shape
        rank = steps * count
        share = rows // n_orb
        plan = layout(rank, count, depth, n_grid)
        groups, tiles, cuts = plan
        n_groups = len(groups)
        n_pieces = len(pieces_of(share))
        wide = steps * 128
        corners = steps * (steps + 1) // 2
        assert count < 128 and count % BLOCK == 0 and corners % 2 == 0
        dma = pltpu.SemaphoreType.DMA
        vmem = pltpu.VMEM
        blocks = [vmem((r * tiles, size, 128), BF16) for r, size in cuts]
        factor, diagonal, peaks = pl.pallas_call(
            functools.partial(kernel, n_grid, n_orb, steps, depth * n_orb, plan),
            out_shape=(
                jax.ShapeDtypeStruct((rank, share), F32),
                jax.ShapeDtypeStruct((1, share), F32),
                jax.ShapeDtypeStruct((8, 128), F32),
            ),
            in_specs=[
                pl.BlockSpec(memory_space=pltpu.HBM),
                pl.BlockSpec(memory_space=pltpu.HBM),
            ],
            out_specs=(
                pl.BlockSpec(memory_space=pl.ANY),
                pl.BlockSpec(memory_space=vmem),
                pl.BlockSpec(memory_space=vmem),
            ),
            scratch_shapes=[
                vmem((steps, count), jnp.int32),
                vmem((n_orb, depth, share), BF16),
                vmem((2, depth, share), BF16),
                blocks,
                blocks,
                [vmem((n_grid, size, 128), BF16) for _, size in cuts],
                blocks,
                vmem((rank, share), jnp.int16),
                vmem((rank, share), jnp.int16),
                vmem((1, n_groups * share), F32),
                vmem((1, n_groups * share), F32),
                vmem((1, 2 * share), F32),
                vmem((1, 2 * share), F32),
                vmem((rank, share), F32),
                vmem((1, share), F32),
                vmem((2, corners // 2, count, 128), F32),
                vmem((2, corners // 2, count, 128), F32),
                vmem((rank, wide), F32),
                vmem((rank, share), F32),
                vmem((2, 8, 128), F32),
                vmem((n_orb, 8, 128), F32),
                vmem((n_grid, 8, 128), F32),
                dma, dma((n_orb,)), dma((n_pieces,)), dma((2,)), dma((2,)),
                dma((n_groups, n_grid)), dma((n_groups, n_grid)),
                dma((n_groups, n_grid)), dma((n_groups, n_grid)),
                dma((n_groups,)), dma((n_groups,)), dma, dma, dma, dma,
                dma((n_groups, n_pieces)), dma((n_groups, n_pieces)),
                dma((n_groups, n_pieces)), dma((n_groups, n_pieces)),
                dma, dma,
                dma((n_orb,)), dma((n_orb,)), dma((n_grid,)), dma((n_grid,)),
            ],
            compiler_params=pltpu.CompilerParams(
                collective_id=0, has_side_effects=True, vmem_limit_bytes=46 * 1024 * 1024
            ),
        )(
            pltpu.with_memory_space_constraint(orbitals, pltpu.HBM),
            pltpu.with_memory_space_constraint(pivots, pltpu.HBM),
        )
        return factor.T, diagonal.reshape(share), peaks[:steps, 0]

    return jax.shard_map(
        on_device,
        mesh=mesh,
        in_specs=(P("orb", "grid"), P()),
        out_specs=(P(("grid", "orb"), None), P(("grid", "orb")), P()),
        check_vma=False,
    )
```

```python
import functools

import jax
import jax.numpy as jnp
from jax import lax
from jax.experimental import pallas as pl
from jax.experimental.pallas import tpu as pltpu
from jax.sharding import PartitionSpec as P

F32 = jnp.float32
BF16 = jnp.bfloat16
HIGHEST = lax.Precision.HIGHEST
MESH = pl.DeviceIdType.MESH
BLOCK = 48
AHEAD = 3
ONE_ROUND = 32


def dot_nn(a, b, precision=None):
    return lax.dot_general(
        a, b, (((1,), (0,)), ((), ())), precision=precision, preferred_element_type=F32
    )


def dot_nt(a, b, precision=None):
    return lax.dot_general(
        a, b, (((1,), (1,)), ((), ())), precision=precision, preferred_element_type=F32
    )


def dot_tn(a, b, precision=None):
    return lax.dot_general(
        a, b, (((0,), (0,)), ((), ())), precision=precision, preferred_element_type=F32
    )


def spread_row(t, r):
    return jnp.broadcast_to(t[r : r + 1, :], (8, 128))


def spread_column(t, c):
    return jnp.broadcast_to(t[:, c : c + 1], (8, 128))


def eliminate(square, wide_rows):
    size = square.shape[0]
    groups = size // 8
    width = wide_rows.shape[1] // 128
    tile = [square[8 * i : 8 * i + 8, :] for i in range(groups)]
    wide = [
        [wide_rows[8 * i : 8 * i + 8, 128 * v : 128 * v + 128] for v in range(width)]
        for i in range(groups)
    ]
    row_at = lax.broadcasted_iota(jnp.int32, (8, 128), 0)
    for j in range(groups):
        columns = [spread_column(tile[j], 8 * j + c) for c in range(8)]
        entry = {(r, c): spread_row(columns[c], r) for r in range(8) for c in range(r + 1)}
        scale, low = [], {}
        for k in range(8):
            s = lax.rsqrt(entry[k, k])
            scale.append(s)
            for r in range(k + 1, 8):
                low[r, k] = entry[r, k] * s
            for r in range(k + 1, 8):
                for c in range(k + 1, r + 1):
                    entry[r, c] = entry[r, c] - low[r, k] * low[c, k]

        def forward(rows):
            done = []
            for k in range(8):
                x = rows[k]
                for c in range(k):
                    x = x - low[k, c] * done[c]
                done.append(x * scale[k])
            return done

        def gather(done):
            out = done[0]
            for k in range(1, 8):
                out = jnp.where(row_at == k, done[k], out)
            return out

        last = j == groups - 1
        fresh_tile = None if last else forward([spread_row(tile[j], k) for k in range(8)])
        fresh_wide = [forward([spread_row(wide[j][v], k) for k in range(8)]) for v in range(width)]
        for i in range(j + 1, groups):
            left = forward([spread_column(tile[i], 8 * j + c) for c in range(8)])
            for k in range(8):
                tile[i] = tile[i] - left[k] * fresh_tile[k]
                for v in range(width):
                    wide[i][v] = wide[i][v] - left[k] * fresh_wide[v][k]
        for v in range(width):
            wide[j][v] = gather(fresh_wide[v])
    return jnp.concatenate([jnp.concatenate(row, axis=1) for row in wide], axis=0)


def layout(rank, count, depth, n_grid):
    groups = [(top, count) for top in range(0, rank, count)]
    tiles = -(-depth // 128)
    cuts = []
    for _, rows in groups:
        parts = max(
            (r for r in range(1, rows // 16 + 1) if r * tiles <= n_grid and rows % (16 * r) == 0),
            default=1,
        )
        cuts.append((parts, rows // parts))
    return groups, tiles, cuts


def pieces_of(share):
    units = share // 128
    sizes = [units * 5 // 16, units * 5 // 16, units * 4 // 16]
    sizes.append(units - sum(sizes))
    starts = [sum(sizes[:i]) for i in range(len(sizes))]
    return [(128 * a, 128 * n) for a, n in zip(starts, sizes) if n]


def kernel(
    n_grid, n_orb, steps, orbitals_count, plan,
    orb_hbm, piv_hbm,
    factor_hbm, diag_ref, peaks_ref,
    piv_ref, own, other, mines, totals, heards, swaps, sums, arrived, scales, far_scales,
    moment, far_moment, local, own_squares, pair_sends, pair_recvs,
    aug, out_v, tile_mine, tile_far,
    piv_sem, load_sem, out_sem, x_send, x_recv, p1_send, p1_recv, p2_send, p2_recv,
    c_send, c_recv, q_send, q_recv, h_send, h_recv, s_send, s_recv, z_send, z_recv,
    m_send, m_recv, mo_send, mo_recv,
):
    groups, tiles, cuts = plan
    g = lax.axis_index("grid")
    o = lax.axis_index("orb")
    core = lax.rem(o, 2)
    side = o // 2
    mate = o + 1 - 2 * core
    across = (1 - side) * 2 + core
    depth, share = own.shape[1], own.shape[2]
    count = piv_ref.shape[1]
    rank = steps * count
    rows = share * n_orb
    pieces = pieces_of(share)
    n_groups = len(groups)
    piv_copy = pltpu.make_async_copy(piv_hbm, piv_ref, piv_sem)
    piv_copy.start()
    loads = [
        pltpu.make_async_copy(
            orb_hbm.at[:, pl.ds(b * share, share)], own.at[b], load_sem.at[b]
        )
        for b in range(n_orb)
    ]
    loads[0].start()

    def partner(d):
        if n_grid & (n_grid - 1):
            return lax.rem(n_grid + d - g, n_grid)
        at = g
        for bit in range(n_grid.bit_length() - 1):
            if d >> bit & 1:
                at = at + (1 - 2 * lax.rem(g // (1 << bit), 2)) * (1 << bit)
        return at

    reach = [
        (dg, do)
        for dg in range(n_grid - 1, -1, -1)
        for do in range(n_orb - 1, -1, -1)
        if (dg or do) and (ONE_ROUND >= n_grid * n_orb or not (dg and do))
    ]

    def far_device(dg, do):
        return (partner(dg) if dg else g, lax.rem(o + do, n_orb) if do else o)

    barrier = pltpu.get_barrier_semaphore()
    for dg, do in reach:
        pl.semaphore_signal(
            barrier, inc=1, device_id=far_device(dg, do), device_id_type=MESH
        )
    piv_copy.wait()
    for copy in loads[1:]:
        copy.start()
    base = g * rows
    flat = jnp.concatenate(
        [piv_ref[...].astype(F32), jnp.zeros((8 - piv_ref.shape[0], count), F32)], axis=0
    ).T
    wanted = (
        jnp.concatenate([flat[:, s : s + 1] for s in range(steps)], axis=0).astype(jnp.int32)
        - base
    )
    picked = None
    for b in range(n_orb):
        loads[b].wait()
        lanes = lax.broadcasted_iota(jnp.int32, (rank, share), 1) + b * share
        hot = jnp.where(lanes == wanted, 1.0, 0.0).astype(BF16)
        term = dot_nt(hot, own[b])
        picked = term if picked is None else picked + term
    picked = jnp.concatenate(
        [picked.astype(BF16), jnp.zeros((rank, tiles * 128 - depth), BF16)], axis=1
    )
    for i, (first_row, _) in enumerate(groups):
        parts, size = cuts[i]
        for q in range(parts * tiles):
            at = first_row + q // tiles * size
            lane = q % tiles * 128
            mines[i][q] = picked[at : at + size, lane : lane + 128]
    pl.semaphore_wait(barrier, len(reach))

    def block_of(i, owner):
        return lax.rem(owner, cuts[i][0] * tiles)

    def owned(i, owner, action):
        if cuts[i][0] * tiles == n_grid:
            action()
        else:
            pl.when(owner < cuts[i][0] * tiles)(action)

    others = range(n_grid - 1, 0, -1)

    def first(i, d):
        target = partner(d)
        return target, pltpu.make_async_remote_copy(
            src_ref=mines[i].at[block_of(i, target)],
            dst_ref=heards[i].at[d],
            send_sem=p1_send.at[i, d],
            recv_sem=p1_recv.at[i, d],
            device_id=(target, o),
            device_id_type=MESH,
        )

    def second(i, d):
        target = partner(d)
        return pltpu.make_async_remote_copy(
            src_ref=heards[i].at[0],
            dst_ref=totals[i].at[block_of(i, g)],
            send_sem=p2_send.at[i, d],
            recv_sem=p2_recv.at[i, d],
            device_id=(target, o),
            device_id_type=MESH,
        )
    def scatter(i):
        for d in others:
            target, copy = first(i, d)
            owned(i, target, copy.start)

    for i in range(min(2, n_groups)):
        scatter(i)

    crossing = []
    for yy in range(2):
        start = pl.multiple_of((yy * 2 + 1 - core) * share, share)
        copy = pltpu.make_async_remote_copy(
            src_ref=orb_hbm.at[:, pl.ds(start, share)],
            dst_ref=other.at[yy],
            send_sem=x_send.at[yy],
            recv_sem=x_recv.at[yy],
            device_id=(g, mate),
            device_id_type=MESH,
        )
        copy.start()
        crossing.append(copy)

    def add_up(i):

        def action():
            added = mines[i][block_of(i, g)]
            for d in reversed(others):
                first(i, d)[1].wait_recv()
                added = added + heards[i][d]
            heards[i][0] = added
            for d in others:
                second(i, d).start()
            totals[i][block_of(i, g)] = added

        owned(i, g, action)
        if i + 2 < n_groups:
            scatter(i + 2)

    for i in range(min(2, n_groups)):
        add_up(i)
    for copy in crossing:
        copy.wait_recv()

    def squares_of(block):
        x = block.astype(F32)
        return jnp.sum(x * x, axis=0, keepdims=True)

    def sum_of(block):
        return jnp.sum(block.astype(F32), axis=0, keepdims=True)

    for lo, n in pieces:
        a, b = own[across, :, lo : lo + n], other[1 - side, :, lo : lo + n]
        moment[:, lo : lo + n] = squares_of(a) + squares_of(b)
        moment[:, share + lo : share + lo + n] = sum_of(a) + sum_of(b)
    moment_copy = pltpu.make_async_remote_copy(
        src_ref=moment, dst_ref=far_moment, send_sem=m_send, recv_sem=m_recv,
        device_id=(g, across), device_id_type=MESH,
    )
    moment_copy.start()

    def gathered(i, ref):
        parts, _ = cuts[i]
        return jnp.concatenate(
            [
                jnp.concatenate([ref[r * tiles + t] for t in range(tiles)], axis=1)
                for r in range(parts)
            ],
            axis=0,
        )[:, 0:depth]

    swapping, here, there, means, pair_copies = [], [], [], [], []
    half = count // 2

    def meet(i):
        for d in reversed(others):
            owned(i, partner(d), second(i, d).wait_recv)
        copy = pltpu.make_async_remote_copy(
            src_ref=totals[i], dst_ref=swaps[i], send_sem=c_send.at[i], recv_sem=c_recv.at[i],
            device_id=(g, mate), device_id_type=MESH,
        )
        copy.start()
        swapping.append(copy)
        here.append(gathered(i, totals[i]))
        if i == 0:
            lo, n = pieces[0]
            out_v[0 : groups[0][1], lo : lo + n] = dot_nn(here[0], own[across, :, lo : lo + n])
        if i + 2 < n_groups:
            add_up(i + 2)
        copy.wait_recv()
        there.append(gathered(i, swaps[i]))
        means.append(
            (
                jnp.sum(here[i].astype(F32), axis=1, keepdims=True)
                + jnp.sum(there[i].astype(F32), axis=1, keepdims=True)
            )
            / (2.0 * depth)
        )
        pair = dot_nt(jnp.concatenate(here, axis=0), here[i]) + dot_nt(
            jnp.concatenate(there, axis=0), there[i]
        )
        for h in range(2):
            for r in range(i + 1):
                top = r * count + h * half
                pair_sends[i][h, r * half : (r + 1) * half, 0:count] = pair[top : top + half]
            pair_sends[i][h, i * half : (i + 1) * half, count : count + 1] = means[i][
                h * half : (h + 1) * half
            ]
        pair_copy = pltpu.make_async_remote_copy(
            src_ref=pair_sends[i].at[core], dst_ref=pair_recvs[i].at[0],
            send_sem=q_send.at[i], recv_sem=q_recv.at[i],
            device_id=(g, across), device_id_type=MESH,
        )
        pair_copy.start()
        pair_copies.append(pair_copy)

    travel = {}

    def code(i, p):
        lo, n = pieces[p]
        top, size = groups[i]
        if i or p:
            inner = dot_nn(here[i], own[across, :, lo : lo + n])
        else:
            inner = out_v[0:size, lo : lo + n]
        inner = inner + dot_nn(there[i], other[1 - side, :, lo : lo + n])
        rest = inner - means[i] * moment[:, share + lo : share + lo + n]
        most = jnp.max(jnp.abs(rest), axis=0, keepdims=True)
        step = jnp.maximum(most * (1.0 / 32767.0), 1e-30)
        coded = jnp.clip(jnp.round(rest * (1.0 / step)), -32767.0, 32767.0)
        sums[top : top + size, lo : lo + n] = coded.astype(jnp.int32).astype(jnp.int16)
        scales[:, i * share + lo : i * share + lo + n] = step

    def send(i, p):
        lo, n = pieces[p]
        top, size = groups[i]
        travel[i, p] = (
            pltpu.make_async_remote_copy(
                src_ref=scales.at[:, pl.ds(i * share + lo, n)],
                dst_ref=far_scales.at[:, pl.ds(i * share + lo, n)],
                send_sem=z_send.at[i, p], recv_sem=z_recv.at[i, p],
                device_id=(g, across), device_id_type=MESH,
            ),
            pltpu.make_async_remote_copy(
                src_ref=sums.at[pl.ds(top, size), pl.ds(lo, n)],
                dst_ref=arrived.at[pl.ds(top, size), pl.ds(lo, n)],
                send_sem=s_send.at[i, p], recv_sem=s_recv.at[i, p],
                device_id=(g, across), device_id_type=MESH,
            ),
        )
        for copy in travel[i, p]:
            copy.start()

    late = n_groups - 1
    held = []
    for i in range(late):
        meet(i)
        for p in range(len(pieces)):
            code(i, p)
            if i * len(pieces) + p < AHEAD:
                send(i, p)
            else:
                held.append((i, p))
    meet(late)

    here_all = jnp.concatenate(here, axis=0)
    there_all = jnp.concatenate(there, axis=0)
    for i, p in held:
        send(i, p)
    for p in range(len(pieces)):
        code(late, p)
        send(late, p)
    for lo, n in pieces:
        a, b = own[o, :, lo : lo + n], other[side, :, lo : lo + n]
        local[:, lo : lo + n] = dot_nn(here_all, a) + dot_nn(there_all, b)
        own_squares[:, lo : lo + n] = squares_of(a) + squares_of(b)
    half_copies = []
    for i in range(n_groups):
        pair_copies[i].wait_recv()
        half_copy = pltpu.make_async_remote_copy(
            src_ref=pair_recvs[i].at[0], dst_ref=pair_recvs[i].at[1],
            send_sem=h_send.at[i], recv_sem=h_recv.at[i],
            device_id=(g, mate), device_id_type=MESH,
        )
        half_copy.start()
        half_copies.append(half_copy)
    wide = aug.shape[1]
    aug[...] = jnp.zeros((rank, wide), F32)
    far_means = []
    for i in range(n_groups):
        half_copies[i].wait_recv()
        for h in range(2):
            far = pair_recvs[i][core if h == 0 else 1 - core]
            entries = jnp.square((pair_sends[i][h] + far)[:, 0:count] / orbitals_count)
            for r in range(i + 1):
                top = r * count + h * half
                aug[top : top + half, 128 * i : 128 * i + count] = entries[
                    r * half : (r + 1) * half
                ]
            far_means.append(far[i * half : (i + 1) * half, count : count + 1])
    far_mean = jnp.concatenate(far_means, axis=0)

    def lane_of(row):
        return row // count * 128 + row % count

    at = lax.broadcasted_iota(jnp.int32, (BLOCK, wide), 1)
    eye_row = lax.broadcasted_iota(jnp.int32, (BLOCK, wide), 0)
    for start in range(0, rank, BLOCK):
        lane = lane_of(start)
        tile = lane // 128 * 128
        strip = jnp.where(at >= lane, aug[start : start + BLOCK, :], 0.0)
        if start:
            done = jnp.concatenate(
                [
                    jnp.where(
                        (at >= lane) | (at < lane_of(i) + BLOCK), aug[i : i + BLOCK, :], 0.0
                    )
                    for i in range(0, start, BLOCK)
                ],
                axis=0,
            )
            above = dot_tn(aug[0:start, tile : tile + 128], done, HIGHEST)
            strip = strip - above[lane - tile : lane - tile + BLOCK, :]
        square = strip[:, tile : tile + 128]
        if lane > tile:
            square = pltpu.roll(square, 128 - (lane - tile), 1)
        unit = jnp.where(at == eye_row + lane, 1.0, 0.0)
        aug[start : start + BLOCK, :] = eliminate(
            square, jnp.where((at >= lane) & (at < lane + BLOCK), unit, strip)
        )
    inverse = []
    for s in range(steps):
        bands = []
        for i in range(s * count, (s + 1) * count, BLOCK):
            bands.append(jnp.where(at < lane_of(i) + BLOCK, aug[i : i + BLOCK, :], 0.0))
        band = jnp.concatenate(bands, axis=0)
        inverse.append(
            jnp.concatenate([band[:, 128 * c : 128 * c + count] for c in range(s + 1)], axis=1)
        )

    best = [None] * steps
    stores = []
    moment_copy.wait_recv()
    whole_rows = orbitals_count * 1.0

    def columns_of(i, lo, n):
        top, size = groups[i]
        inner = (
            local[top : top + size, lo : lo + n]
            + arrived[top : top + size, lo : lo + n].astype(jnp.int32).astype(F32)
            * far_scales[:, i * share + lo : i * share + lo + n]
            + far_mean[top : top + size] * far_moment[:, share + lo : share + lo + n]
        )
        return jnp.square(inner / whole_rows)

    def settle(s, solved, diagonal, lo, n):
        out_v[s * count : (s + 1) * count, lo : lo + n] = solved
        diagonal = diagonal - jnp.sum(solved * solved, axis=0, keepdims=True)
        top = jnp.max(diagonal, axis=1, keepdims=True)
        best[s] = top if best[s] is None else jnp.maximum(best[s], top)
        return diagonal

    for p, (lo, n) in enumerate(pieces):
        for i in range(late):
            for copy in travel[i, p]:
                copy.wait_recv()
        diagonal = jnp.square(
            (own_squares[:, lo : lo + n] + far_moment[:, lo : lo + n]) / whole_rows
        )
        if late:
            columns = jnp.concatenate([columns_of(i, lo, n) for i in range(late)], axis=0)
            for s in range(late):
                solved = dot_nn(inverse[s], columns[0 : (s + 1) * count], HIGHEST)
                diagonal = settle(s, solved, diagonal, lo, n)
            out_v[late * count : rank, lo : lo + n] = dot_nn(
                inverse[late][:, 0 : late * count], columns, HIGHEST
            )
        diag_ref[:, lo : lo + n] = diagonal
    for p, (lo, n) in enumerate(pieces):
        for copy in travel[late, p]:
            copy.wait_recv()
        solved = dot_nn(
            inverse[late][:, late * count : rank], columns_of(late, lo, n), HIGHEST
        )
        if late:
            solved = solved + out_v[late * count : rank, lo : lo + n]
        diag_ref[:, lo : lo + n] = settle(late, solved, diag_ref[:, lo : lo + n], lo, n)
        store = pltpu.make_async_copy(
            out_v.at[:, pl.ds(lo, n)], factor_hbm.at[:, pl.ds(lo, n)], out_sem.at[p]
        )
        store.start()
        stores.append(store)
    row8 = lax.broadcasted_iota(jnp.int32, (8, 128), 0)
    tile = jnp.zeros((8, 128), F32)
    for s in range(steps):
        tile = jnp.where(row8 == s, jnp.broadcast_to(best[s], (8, 128)), tile)
    if ONE_ROUND >= n_grid * n_orb:
        stages = [reach]
    else:
        stages = [[x for x in reach if not x[0]], [x for x in reach if x[0]]]
    rounds = []
    for k, stage in enumerate(stages):
        tile_mine[k] = tile
        started = []
        for dg, do in stage:
            at = dg * n_orb + do
            copy = pltpu.make_async_remote_copy(
                src_ref=tile_mine.at[k], dst_ref=tile_far.at[at],
                send_sem=mo_send.at[at], recv_sem=mo_recv.at[at],
                device_id=far_device(dg, do), device_id_type=MESH,
            )
            copy.start()
            started.append((at, copy))
        for at, copy in reversed(started):
            copy.wait_recv()
            tile = jnp.maximum(tile, tile_far[at])
        rounds += [copy for _, copy in started]
    peaks_ref[...] = tile
    for store in stores:
        store.wait()
    for i in range(n_groups):
        for d in others:
            target, copy = first(i, d)
            owned(i, target, copy.wait_send)

        def sent(i=i):
            for d in others:
                second(i, d).wait_send()

        owned(i, g, sent)

    for copy in crossing + swapping + [moment_copy] + pair_copies + half_copies + rounds:
        copy.wait_send()
    for pair_of in travel.values():
        for copy in pair_of:
            copy.wait_send()


def solution(mesh):
    n_grid, n_orb = mesh.shape["grid"], mesh.shape["orb"]
    assert n_orb == 4

    def on_device(orbitals, pivots):
        depth, rows = orbitals.shape
        steps, count = pivots.shape
        rank = steps * count
        share = rows // n_orb
        plan = layout(rank, count, depth, n_grid)
        groups, tiles, cuts = plan
        n_groups = len(groups)
        n_pieces = len(pieces_of(share))
        wide = steps * 128
        assert count < 128 and count % BLOCK == 0 and count % 16 == 0
        dma = pltpu.SemaphoreType.DMA
        vmem = pltpu.VMEM
        corners = [vmem((2, (i + 1) * count // 2, 128), F32) for i in range(n_groups)]
        blocks = [vmem((r * tiles, size, 128), BF16) for r, size in cuts]
        factor, diagonal, peaks = pl.pallas_call(
            functools.partial(kernel, n_grid, n_orb, steps, depth * n_orb, plan),
            out_shape=(
                jax.ShapeDtypeStruct((rank, share), F32),
                jax.ShapeDtypeStruct((1, share), F32),
                jax.ShapeDtypeStruct((8, 128), F32),
            ),
            in_specs=[
                pl.BlockSpec(memory_space=pltpu.HBM),
                pl.BlockSpec(memory_space=pltpu.HBM),
            ],
            out_specs=(
                pl.BlockSpec(memory_space=pl.ANY),
                pl.BlockSpec(memory_space=vmem),
                pl.BlockSpec(memory_space=vmem),
            ),
            scratch_shapes=[
                vmem((steps, count), jnp.int32),
                vmem((n_orb, depth, share), BF16),
                vmem((2, depth, share), BF16),
                blocks,
                blocks,
                [vmem((n_grid, size, 128), BF16) for _, size in cuts],
                blocks,
                vmem((rank, share), jnp.int16),
                vmem((rank, share), jnp.int16),
                vmem((1, n_groups * share), F32),
                vmem((1, n_groups * share), F32),
                vmem((1, 2 * share), F32),
                vmem((1, 2 * share), F32),
                vmem((rank, share), F32),
                vmem((1, share), F32),
                corners,
                corners,
                vmem((rank, wide), F32),
                vmem((rank, share), F32),
                vmem((2, 8, 128), F32),
                vmem((n_grid * n_orb, 8, 128), F32),
                dma, dma((n_orb,)), dma((n_pieces,)), dma((2,)), dma((2,)),
                dma((n_groups, n_grid)), dma((n_groups, n_grid)),
                dma((n_groups, n_grid)), dma((n_groups, n_grid)),
                dma((n_groups,)), dma((n_groups,)),
                dma((n_groups,)), dma((n_groups,)), dma((n_groups,)), dma((n_groups,)),
                dma((n_groups, n_pieces)), dma((n_groups, n_pieces)),
                dma((n_groups, n_pieces)), dma((n_groups, n_pieces)),
                dma, dma,
                dma((n_grid * n_orb,)), dma((n_grid * n_orb,)),
            ],
            compiler_params=pltpu.CompilerParams(
                collective_id=0, has_side_effects=True, vmem_limit_bytes=46 * 1024 * 1024
            ),
        )(
            pltpu.with_memory_space_constraint(orbitals, pltpu.HBM),
            pltpu.with_memory_space_constraint(pivots, pltpu.HBM),
        )
        return factor.T, diagonal.reshape(share), peaks[:steps, 0]

    return jax.shard_map(
        on_device,
        mesh=mesh,
        in_specs=(P("orb", "grid"), P()),
        out_specs=(P(("grid", "orb"), None), P(("grid", "orb")), P()),
        check_vma=False,
    )
```

```python
import functools

import jax
import jax.numpy as jnp
from jax import lax
from jax.experimental import pallas as pl
from jax.experimental.pallas import tpu as pltpu
from jax.sharding import PartitionSpec as P

F32 = jnp.float32
BF16 = jnp.bfloat16
HIGHEST = lax.Precision.HIGHEST
MESH = pl.DeviceIdType.MESH
BLOCK = 48
AHEAD = 3
ONE_ROUND = 32


def dot_nn(a, b, precision=None):
    return lax.dot_general(
        a, b, (((1,), (0,)), ((), ())), precision=precision, preferred_element_type=F32
    )


def dot_nt(a, b, precision=None):
    return lax.dot_general(
        a, b, (((1,), (1,)), ((), ())), precision=precision, preferred_element_type=F32
    )


def dot_tn(a, b, precision=None):
    return lax.dot_general(
        a, b, (((0,), (0,)), ((), ())), precision=precision, preferred_element_type=F32
    )


def spread_row(t, r):
    return jnp.broadcast_to(t[r : r + 1, :], (8, 128))


def spread_column(t, c):
    return jnp.broadcast_to(t[:, c : c + 1], (8, 128))


def eliminate(square, wide_rows):
    size = square.shape[0]
    groups = size // 8
    width = wide_rows.shape[1] // 128
    tile = [square[8 * i : 8 * i + 8, :] for i in range(groups)]
    wide = [
        [wide_rows[8 * i : 8 * i + 8, 128 * v : 128 * v + 128] for v in range(width)]
        for i in range(groups)
    ]
    row_at = lax.broadcasted_iota(jnp.int32, (8, 128), 0)
    for j in range(groups):
        columns = [spread_column(tile[j], 8 * j + c) for c in range(8)]
        entry = {(r, c): spread_row(columns[c], r) for r in range(8) for c in range(r + 1)}
        scale, low = [], {}
        for k in range(8):
            s = lax.rsqrt(entry[k, k])
            scale.append(s)
            for r in range(k + 1, 8):
                low[r, k] = entry[r, k] * s
            for r in range(k + 1, 8):
                for c in range(k + 1, r + 1):
                    entry[r, c] = entry[r, c] - low[r, k] * low[c, k]

        def forward(rows):
            done = []
            for k in range(8):
                x = rows[k]
                for c in range(k):
                    x = x - low[k, c] * done[c]
                done.append(x * scale[k])
            return done

        def gather(done):
            out = done[0]
            for k in range(1, 8):
                out = jnp.where(row_at == k, done[k], out)
            return out

        last = j == groups - 1
        fresh_tile = None if last else forward([spread_row(tile[j], k) for k in range(8)])
        fresh_wide = [forward([spread_row(wide[j][v], k) for k in range(8)]) for v in range(width)]
        for i in range(j + 1, groups):
            left = forward([spread_column(tile[i], 8 * j + c) for c in range(8)])
            for k in range(8):
                tile[i] = tile[i] - left[k] * fresh_tile[k]
                for v in range(width):
                    wide[i][v] = wide[i][v] - left[k] * fresh_wide[v][k]
        for v in range(width):
            wide[j][v] = gather(fresh_wide[v])
    return jnp.concatenate([jnp.concatenate(row, axis=1) for row in wide], axis=0)


def layout(rank, count, depth, n_grid):
    groups = [(top, count) for top in range(0, rank, count)]
    tiles = -(-depth // 128)
    cuts = []
    for _, rows in groups:
        parts = max(
            (r for r in range(1, rows // 16 + 1) if r * tiles <= n_grid and rows % (16 * r) == 0),
            default=1,
        )
        cuts.append((parts, rows // parts))
    return groups, tiles, cuts


def pieces_of(share):
    units = share // 128
    sizes = [units * 5 // 16, units * 5 // 16, units * 4 // 16]
    sizes.append(units - sum(sizes))
    starts = [sum(sizes[:i]) for i in range(len(sizes))]
    return [(128 * a, 128 * n) for a, n in zip(starts, sizes) if n]


def kernel(
    n_grid, n_orb, steps, orbitals_count, plan,
    orb_hbm, piv_hbm,
    factor_hbm, diag_ref, peaks_ref,
    piv_ref, own, other, mines, totals, heards, swaps, sums, arrived, scales, far_scales,
    moment, far_moment, local, own_squares, pair_sends, pair_recvs,
    aug, out_v, tile_mine, tile_far,
    piv_sem, load_sem, out_sem, x_send, x_recv, p1_send, p1_recv, p2_send, p2_recv,
    c_send, c_recv, q_send, q_recv, h_send, h_recv, s_send, s_recv, z_send, z_recv,
    m_send, m_recv, mo_send, mo_recv,
):
    groups, tiles, cuts = plan
    g = lax.axis_index("grid")
    o = lax.axis_index("orb")
    core = lax.rem(o, 2)
    side = o // 2
    mate = o + 1 - 2 * core
    across = (1 - side) * 2 + core
    depth, share = own.shape[1], own.shape[2]
    count = piv_ref.shape[1]
    rank = steps * count
    rows = share * n_orb
    pieces = pieces_of(share)
    n_groups = len(groups)
    piv_copy = pltpu.make_async_copy(piv_hbm, piv_ref, piv_sem)
    piv_copy.start()
    loads = [
        pltpu.make_async_copy(
            orb_hbm.at[:, pl.ds(b * share, share)], own.at[b], load_sem.at[b]
        )
        for b in range(n_orb)
    ]
    loads[0].start()

    def partner(d):
        if n_grid & (n_grid - 1):
            return lax.rem(n_grid + d - g, n_grid)
        at = g
        for bit in range(n_grid.bit_length() - 1):
            if d >> bit & 1:
                at = at + (1 - 2 * lax.rem(g // (1 << bit), 2)) * (1 << bit)
        return at

    reach = [
        (dg, do)
        for dg in range(n_grid - 1, -1, -1)
        for do in range(n_orb - 1, -1, -1)
        if (dg or do) and (ONE_ROUND >= n_grid * n_orb or not (dg and do))
    ]

    def far_device(dg, do):
        return (partner(dg) if dg else g, lax.rem(o + do, n_orb) if do else o)

    barrier = pltpu.get_barrier_semaphore()
    for dg, do in reach:
        pl.semaphore_signal(
            barrier, inc=1, device_id=far_device(dg, do), device_id_type=MESH
        )
    piv_copy.wait()
    for copy in loads[1:]:
        copy.start()
    base = g * rows
    flat = jnp.concatenate(
        [piv_ref[...].astype(F32), jnp.zeros((8 - piv_ref.shape[0], count), F32)], axis=0
    ).T
    wanted = (
        jnp.concatenate([flat[:, s : s + 1] for s in range(steps)], axis=0).astype(jnp.int32)
        - base
    )
    picked = None
    for b in range(n_orb):
        loads[b].wait()
        lanes = lax.broadcasted_iota(jnp.int32, (rank, share), 1) + b * share
        hot = jnp.where(lanes == wanted, 1.0, 0.0).astype(BF16)
        term = dot_nt(hot, own[b])
        picked = term if picked is None else picked + term
    picked = jnp.concatenate(
        [picked.astype(BF16), jnp.zeros((rank, tiles * 128 - depth), BF16)], axis=1
    )
    for i, (first_row, _) in enumerate(groups):
        parts, size = cuts[i]
        for q in range(parts * tiles):
            at = first_row + q // tiles * size
            lane = q % tiles * 128
            mines[i][q] = picked[at : at + size, lane : lane + 128]
    pl.semaphore_wait(barrier, len(reach))

    def block_of(i, owner):
        return lax.rem(owner, cuts[i][0] * tiles)

    def owned(i, owner, action):
        if cuts[i][0] * tiles == n_grid:
            action()
        else:
            pl.when(owner < cuts[i][0] * tiles)(action)

    others = range(n_grid - 1, 0, -1)

    def first(i, d):
        target = partner(d)
        return target, pltpu.make_async_remote_copy(
            src_ref=mines[i].at[block_of(i, target)],
            dst_ref=heards[i].at[d],
            send_sem=p1_send.at[i, d],
            recv_sem=p1_recv.at[i, d],
            device_id=(target, o),
            device_id_type=MESH,
        )

    def second(i, d):
        target = partner(d)
        return pltpu.make_async_remote_copy(
            src_ref=heards[i].at[0],
            dst_ref=totals[i].at[block_of(i, g)],
            send_sem=p2_send.at[i, d],
            recv_sem=p2_recv.at[i, d],
            device_id=(target, o),
            device_id_type=MESH,
        )
    def scatter(i):
        for d in others:
            target, copy = first(i, d)
            owned(i, target, copy.start)

    for i in range(min(2, n_groups)):
        scatter(i)

    crossing = []
    for yy in range(2):
        start = pl.multiple_of((yy * 2 + 1 - core) * share, share)
        copy = pltpu.make_async_remote_copy(
            src_ref=orb_hbm.at[:, pl.ds(start, share)],
            dst_ref=other.at[yy],
            send_sem=x_send.at[yy],
            recv_sem=x_recv.at[yy],
            device_id=(g, mate),
            device_id_type=MESH,
        )
        copy.start()
        crossing.append(copy)

    def add_up(i):

        def action():
            added = mines[i][block_of(i, g)]
            for d in reversed(others):
                first(i, d)[1].wait_recv()
                added = added + heards[i][d]
            heards[i][0] = added
            for d in others:
                second(i, d).start()
            totals[i][block_of(i, g)] = added

        owned(i, g, action)
        if i + 2 < n_groups:
            scatter(i + 2)

    for i in range(min(2, n_groups)):
        add_up(i)
    for copy in crossing:
        copy.wait_recv()

    def squares_of(block):
        x = block.astype(F32)
        return jnp.sum(x * x, axis=0, keepdims=True)

    def sum_of(block):
        return jnp.sum(block.astype(F32), axis=0, keepdims=True)

    for lo, n in pieces:
        a, b = own[across, :, lo : lo + n], other[1 - side, :, lo : lo + n]
        moment[:, lo : lo + n] = squares_of(a) + squares_of(b)
        moment[:, share + lo : share + lo + n] = sum_of(a) + sum_of(b)
    moment_copy = pltpu.make_async_remote_copy(
        src_ref=moment, dst_ref=far_moment, send_sem=m_send, recv_sem=m_recv,
        device_id=(g, across), device_id_type=MESH,
    )
    moment_copy.start()

    def gathered(i, ref):
        parts, _ = cuts[i]
        return jnp.concatenate(
            [
                jnp.concatenate([ref[r * tiles + t] for t in range(tiles)], axis=1)
                for r in range(parts)
            ],
            axis=0,
        )[:, 0:depth]

    swapping, here, there, means, pair_copies = [], [], [], [], []
    half = count // 2

    def meet(i):
        for d in reversed(others):
            owned(i, partner(d), second(i, d).wait_recv)
        copy = pltpu.make_async_remote_copy(
            src_ref=totals[i], dst_ref=swaps[i], send_sem=c_send.at[i], recv_sem=c_recv.at[i],
            device_id=(g, mate), device_id_type=MESH,
        )
        copy.start()
        swapping.append(copy)
        here.append(gathered(i, totals[i]))
        if i == 0:
            lo, n = pieces[0]
            out_v[0 : groups[0][1], lo : lo + n] = dot_nn(here[0], own[across, :, lo : lo + n])
        copy.wait_recv()
        there.append(gathered(i, swaps[i]))
        means.append(
            (
                jnp.sum(here[i].astype(F32), axis=1, keepdims=True)
                + jnp.sum(there[i].astype(F32), axis=1, keepdims=True)
            )
            / (2.0 * depth)
        )
        pair = dot_nt(jnp.concatenate(here, axis=0), here[i]) + dot_nt(
            jnp.concatenate(there, axis=0), there[i]
        )
        for h in range(2):
            for r in range(i + 1):
                top = r * count + h * half
                pair_sends[i][h, r * half : (r + 1) * half, 0:count] = pair[top : top + half]
            pair_sends[i][h, i * half : (i + 1) * half, count : count + 1] = means[i][
                h * half : (h + 1) * half
            ]
        pair_copy = pltpu.make_async_remote_copy(
            src_ref=pair_sends[i].at[core], dst_ref=pair_recvs[i].at[0],
            send_sem=q_send.at[i], recv_sem=q_recv.at[i],
            device_id=(g, across), device_id_type=MESH,
        )
        pair_copy.start()
        pair_copies.append(pair_copy)

    travel = {}

    def code(i, p):
        lo, n = pieces[p]
        top, size = groups[i]
        if i or p:
            inner = dot_nn(here[i], own[across, :, lo : lo + n])
        else:
            inner = out_v[0:size, lo : lo + n]
        inner = inner + dot_nn(there[i], other[1 - side, :, lo : lo + n])
        rest = inner - means[i] * moment[:, share + lo : share + lo + n]
        most = jnp.max(jnp.abs(rest), axis=0, keepdims=True)
        step = jnp.maximum(most * (1.0 / 32767.0), 1e-30)
        coded = jnp.clip(jnp.round(rest * (1.0 / step)), -32767.0, 32767.0)
        sums[top : top + size, lo : lo + n] = coded.astype(jnp.int32).astype(jnp.int16)
        scales[:, i * share + lo : i * share + lo + n] = step

    def send(i, p):
        lo, n = pieces[p]
        top, size = groups[i]
        travel[i, p] = (
            pltpu.make_async_remote_copy(
                src_ref=scales.at[:, pl.ds(i * share + lo, n)],
                dst_ref=far_scales.at[:, pl.ds(i * share + lo, n)],
                send_sem=z_send.at[i, p], recv_sem=z_recv.at[i, p],
                device_id=(g, across), device_id_type=MESH,
            ),
            pltpu.make_async_remote_copy(
                src_ref=sums.at[pl.ds(top, size), pl.ds(lo, n)],
                dst_ref=arrived.at[pl.ds(top, size), pl.ds(lo, n)],
                send_sem=s_send.at[i, p], recv_sem=s_recv.at[i, p],
                device_id=(g, across), device_id_type=MESH,
            ),
        )
        for copy in travel[i, p]:
            copy.start()

    late = n_groups - 1
    held = []
    for i in range(late):
        meet(i)
        for p in range(len(pieces)):
            code(i, p)
            if i * len(pieces) + p < AHEAD:
                send(i, p)
            else:
                held.append((i, p))
            if p == 0 and i + 2 < n_groups:
                add_up(i + 2)
    meet(late)

    here_all = jnp.concatenate(here, axis=0)
    there_all = jnp.concatenate(there, axis=0)
    for i, p in held:
        send(i, p)
    for p in range(len(pieces)):
        code(late, p)
        send(late, p)
    for lo, n in pieces:
        a, b = own[o, :, lo : lo + n], other[side, :, lo : lo + n]
        local[:, lo : lo + n] = dot_nn(here_all, a) + dot_nn(there_all, b)
        own_squares[:, lo : lo + n] = squares_of(a) + squares_of(b)
    half_copies = []
    for i in range(n_groups):
        pair_copies[i].wait_recv()
        half_copy = pltpu.make_async_remote_copy(
            src_ref=pair_recvs[i].at[0], dst_ref=pair_recvs[i].at[1],
            send_sem=h_send.at[i], recv_sem=h_recv.at[i],
            device_id=(g, mate), device_id_type=MESH,
        )
        half_copy.start()
        half_copies.append(half_copy)
    wide = aug.shape[1]
    aug[...] = jnp.zeros((rank, wide), F32)
    far_means = []
    for i in range(n_groups):
        half_copies[i].wait_recv()
        for h in range(2):
            far = pair_recvs[i][core if h == 0 else 1 - core]
            entries = jnp.square((pair_sends[i][h] + far)[:, 0:count] / orbitals_count)
            for r in range(i + 1):
                top = r * count + h * half
                aug[top : top + half, 128 * i : 128 * i + count] = entries[
                    r * half : (r + 1) * half
                ]
            far_means.append(far[i * half : (i + 1) * half, count : count + 1])
    far_mean = jnp.concatenate(far_means, axis=0)

    def lane_of(row):
        return row // count * 128 + row % count

    at = lax.broadcasted_iota(jnp.int32, (BLOCK, wide), 1)
    eye_row = lax.broadcasted_iota(jnp.int32, (BLOCK, wide), 0)
    for start in range(0, rank, BLOCK):
        lane = lane_of(start)
        tile = lane // 128 * 128
        strip = jnp.where(at >= lane, aug[start : start + BLOCK, :], 0.0)
        if start:
            done = jnp.concatenate(
                [
                    jnp.where(
                        (at >= lane) | (at < lane_of(i) + BLOCK), aug[i : i + BLOCK, :], 0.0
                    )
                    for i in range(0, start, BLOCK)
                ],
                axis=0,
            )
            above = dot_tn(aug[0:start, tile : tile + 128], done, HIGHEST)
            strip = strip - above[lane - tile : lane - tile + BLOCK, :]
        square = strip[:, tile : tile + 128]
        if lane > tile:
            square = pltpu.roll(square, 128 - (lane - tile), 1)
        unit = jnp.where(at == eye_row + lane, 1.0, 0.0)
        aug[start : start + BLOCK, :] = eliminate(
            square, jnp.where((at >= lane) & (at < lane + BLOCK), unit, strip)
        )
    inverse = []
    for s in range(steps):
        bands = []
        for i in range(s * count, (s + 1) * count, BLOCK):
            bands.append(jnp.where(at < lane_of(i) + BLOCK, aug[i : i + BLOCK, :], 0.0))
        band = jnp.concatenate(bands, axis=0)
        inverse.append(
            jnp.concatenate([band[:, 128 * c : 128 * c + count] for c in range(s + 1)], axis=1)
        )

    best = [None] * steps
    stores = []
    moment_copy.wait_recv()
    whole_rows = orbitals_count * 1.0

    def columns_of(i, lo, n):
        top, size = groups[i]
        inner = (
            local[top : top + size, lo : lo + n]
            + arrived[top : top + size, lo : lo + n].astype(jnp.int32).astype(F32)
            * far_scales[:, i * share + lo : i * share + lo + n]
            + far_mean[top : top + size] * far_moment[:, share + lo : share + lo + n]
        )
        return jnp.square(inner / whole_rows)

    def settle(s, solved, diagonal, lo, n):
        out_v[s * count : (s + 1) * count, lo : lo + n] = solved
        diagonal = diagonal - jnp.sum(solved * solved, axis=0, keepdims=True)
        top = jnp.max(diagonal, axis=1, keepdims=True)
        best[s] = top if best[s] is None else jnp.maximum(best[s], top)
        return diagonal

    for p, (lo, n) in enumerate(pieces):
        for i in range(late):
            for copy in travel[i, p]:
                copy.wait_recv()
        diagonal = jnp.square(
            (own_squares[:, lo : lo + n] + far_moment[:, lo : lo + n]) / whole_rows
        )
        if late:
            columns = jnp.concatenate([columns_of(i, lo, n) for i in range(late)], axis=0)
            for s in range(late):
                solved = dot_nn(inverse[s], columns[0 : (s + 1) * count], HIGHEST)
                diagonal = settle(s, solved, diagonal, lo, n)
            out_v[late * count : rank, lo : lo + n] = dot_nn(
                inverse[late][:, 0 : late * count], columns, HIGHEST
            )
        diag_ref[:, lo : lo + n] = diagonal
    for p, (lo, n) in enumerate(pieces):
        for copy in travel[late, p]:
            copy.wait_recv()
        solved = dot_nn(
            inverse[late][:, late * count : rank], columns_of(late, lo, n), HIGHEST
        )
        if late:
            solved = solved + out_v[late * count : rank, lo : lo + n]
        diag_ref[:, lo : lo + n] = settle(late, solved, diag_ref[:, lo : lo + n], lo, n)
        store = pltpu.make_async_copy(
            out_v.at[:, pl.ds(lo, n)], factor_hbm.at[:, pl.ds(lo, n)], out_sem.at[p]
        )
        store.start()
        stores.append(store)
    row8 = lax.broadcasted_iota(jnp.int32, (8, 128), 0)
    tile = jnp.zeros((8, 128), F32)
    for s in range(steps):
        tile = jnp.where(row8 == s, jnp.broadcast_to(best[s], (8, 128)), tile)
    if ONE_ROUND >= n_grid * n_orb:
        stages = [reach]
    else:
        stages = [[x for x in reach if not x[0]], [x for x in reach if x[0]]]
    rounds = []
    for k, stage in enumerate(stages):
        tile_mine[k] = tile
        started = []
        for dg, do in stage:
            at = dg * n_orb + do
            copy = pltpu.make_async_remote_copy(
                src_ref=tile_mine.at[k], dst_ref=tile_far.at[at],
                send_sem=mo_send.at[at], recv_sem=mo_recv.at[at],
                device_id=far_device(dg, do), device_id_type=MESH,
            )
            copy.start()
            started.append((at, copy))
        for at, copy in reversed(started):
            copy.wait_recv()
            tile = jnp.maximum(tile, tile_far[at])
        rounds += [copy for _, copy in started]
    peaks_ref[...] = tile
    for store in stores:
        store.wait()
    for i in range(n_groups):
        for d in others:
            target, copy = first(i, d)
            owned(i, target, copy.wait_send)

        def sent(i=i):
            for d in others:
                second(i, d).wait_send()

        owned(i, g, sent)

    for copy in crossing + swapping + [moment_copy] + pair_copies + half_copies + rounds:
        copy.wait_send()
    for pair_of in travel.values():
        for copy in pair_of:
            copy.wait_send()


def solution(mesh):
    n_grid, n_orb = mesh.shape["grid"], mesh.shape["orb"]
    assert n_orb == 4

    def on_device(orbitals, pivots):
        depth, rows = orbitals.shape
        steps, count = pivots.shape
        rank = steps * count
        share = rows // n_orb
        plan = layout(rank, count, depth, n_grid)
        groups, tiles, cuts = plan
        n_groups = len(groups)
        n_pieces = len(pieces_of(share))
        wide = steps * 128
        assert count < 128 and count % BLOCK == 0 and count % 16 == 0
        dma = pltpu.SemaphoreType.DMA
        vmem = pltpu.VMEM
        corners = [vmem((2, (i + 1) * count // 2, 128), F32) for i in range(n_groups)]
        blocks = [vmem((r * tiles, size, 128), BF16) for r, size in cuts]
        factor, diagonal, peaks = pl.pallas_call(
            functools.partial(kernel, n_grid, n_orb, steps, depth * n_orb, plan),
            out_shape=(
                jax.ShapeDtypeStruct((rank, share), F32),
                jax.ShapeDtypeStruct((1, share), F32),
                jax.ShapeDtypeStruct((8, 128), F32),
            ),
            in_specs=[
                pl.BlockSpec(memory_space=pltpu.HBM),
                pl.BlockSpec(memory_space=pltpu.HBM),
            ],
            out_specs=(
                pl.BlockSpec(memory_space=pl.ANY),
                pl.BlockSpec(memory_space=vmem),
                pl.BlockSpec(memory_space=vmem),
            ),
            scratch_shapes=[
                vmem((steps, count), jnp.int32),
                vmem((n_orb, depth, share), BF16),
                vmem((2, depth, share), BF16),
                blocks,
                blocks,
                [vmem((n_grid, size, 128), BF16) for _, size in cuts],
                blocks,
                vmem((rank, share), jnp.int16),
                vmem((rank, share), jnp.int16),
                vmem((1, n_groups * share), F32),
                vmem((1, n_groups * share), F32),
                vmem((1, 2 * share), F32),
                vmem((1, 2 * share), F32),
                vmem((rank, share), F32),
                vmem((1, share), F32),
                corners,
                corners,
                vmem((rank, wide), F32),
                vmem((rank, share), F32),
                vmem((2, 8, 128), F32),
                vmem((n_grid * n_orb, 8, 128), F32),
                dma, dma((n_orb,)), dma((n_pieces,)), dma((2,)), dma((2,)),
                dma((n_groups, n_grid)), dma((n_groups, n_grid)),
                dma((n_groups, n_grid)), dma((n_groups, n_grid)),
                dma((n_groups,)), dma((n_groups,)),
                dma((n_groups,)), dma((n_groups,)), dma((n_groups,)), dma((n_groups,)),
                dma((n_groups, n_pieces)), dma((n_groups, n_pieces)),
                dma((n_groups, n_pieces)), dma((n_groups, n_pieces)),
                dma, dma,
                dma((n_grid * n_orb,)), dma((n_grid * n_orb,)),
            ],
            compiler_params=pltpu.CompilerParams(
                collective_id=0, has_side_effects=True, vmem_limit_bytes=46 * 1024 * 1024
            ),
        )(
            pltpu.with_memory_space_constraint(orbitals, pltpu.HBM),
            pltpu.with_memory_space_constraint(pivots, pltpu.HBM),
        )
        return factor.T, diagonal.reshape(share), peaks[:steps, 0]

    return jax.shard_map(
        on_device,
        mesh=mesh,
        in_specs=(P("orb", "grid"), P()),
        out_specs=(P(("grid", "orb"), None), P(("grid", "orb")), P()),
        check_vma=False,
    )
```
